32 devices in a mesh: cp: 8 (over z, y), fsdp: 4 (over x, core).
Axes of the slice: x: 2, y: 2, z: 4, core: 2. Of those that a mesh axis runs over, the one named last changes fastest.
Arguments:
- query_states: bfloat16 [4, 1024, 1024], P('fsdp', 'cp'), may hold values from -32 to 32
- key_states: bfloat16 [4, 1024, 1024], P('fsdp', 'cp'), may hold values from -32 to 32
- value_states: bfloat16 [4, 1024, 1024], P('fsdp', 'cp'), may hold values from -6 to 6
- span_order: int32 [16], replicated, may hold values from 0 to 15, as said below
- block_mask: int32 [16, 16], replicated, may hold values from 0 to 1, as said below
- output_weight: bfloat16 [1024, 2048], P(('cp', 'fsdp')), may hold values from -0.1875 to 0.1875
- upstream: bfloat16 [4, 1024, 2048], P('fsdp', 'cp'), may hold values from -6 to 6
Outputs:
- projected: bfloat16 [4, 1024, 2048], P('fsdp', 'cp')
- query_gradient: bfloat16 [4, 1024, 1024], P('fsdp', 'cp')
- key_gradient: bfloat16 [4, 1024, 1024], P('fsdp', 'cp')
- value_gradient: bfloat16 [4, 1024, 1024], P('fsdp', 'cp')
- weight_gradient: float32 [1024, 2048], P(('cp', 'fsdp'))
The draws below stay inside these ranges and needn't reach their ends.
Inputs may be any that keep to these rules, and one draw needn't show every extreme that they name: `span_order`: entries 2 d and 2 d + 1 hold positions p and 15 - p; every position appears once. `block_mask`: the diagonal is 1.
All inputs are finite; a program needn't handle non-finite values.
Results may differ from the reference program's by a relative error of at most 0.024.
Values may be sent and summed in bfloat16 or wider, within the bound.
A program may use at most 128 MiB of HBM per device.

```python
import jax
import jax.numpy as jnp
from jax import lax

D = 2048
HEADS = 8
HEAD = 128
TOK_DEV = 128
HD = 1024
CH = 64
NCH = 16
LEN = 1024
SEQS = 4
N_CP = 8


def base_draw(key, salt):
    subkey = jax.random.fold_in(key, salt)
    values = jnp.clip(5.0 * jax.random.normal(subkey, (SEQS, LEN, HEADS * HEAD), jnp.float32), -32.0, 32.0)
    return values


def draw_query_states(key, part):
    values = base_draw(key, 11)
    return values.astype(jnp.bfloat16)


def draw_key_states(key, part):
    values = base_draw(key, 23)
    return values.astype(jnp.bfloat16)


def draw_span_order(key, part):
    pair_count = NCH // 2
    shuffled = jax.random.permutation(key, pair_count)
    paired = jnp.stack([shuffled, NCH - 1 - shuffled], axis=1).reshape(NCH)
    return paired.astype(jnp.int32)


def draw_block_mask(key, part):
    random_bits = jax.random.randint(key, (NCH, NCH), 0, 2)
    diagonal = jnp.arange(NCH)[:, None] == jnp.arange(NCH)[None, :]
    return jnp.where(diagonal, 1, random_bits).astype(jnp.int32)


def block_scale(rng, extent, pieces, least, top_value):
    def one(dim, blocks):
        draws = jax.random.uniform(jax.random.fold_in(jax.random.fold_in(rng, 6), dim), (blocks,), jnp.float32, least / len(pieces), top_value / len(pieces))
        return jnp.repeat(jnp.exp(draws), extent[dim] // blocks).reshape((-1,) + (1,) * (len(extent) - dim - 1))

    factor_of = one(*pieces[0])
    for cut in pieces[1:]:
        factor_of = factor_of * one(*cut)
    return factor_of


def normal_values(rng, dims, width, most, shards=(), kind=jnp.bfloat16):
    values = width * jax.random.normal(rng, dims, jnp.float32)
    if shards:
        values = values * block_scale(rng, dims, shards, -0.22, 0.18)
    return jnp.clip(values, -most, most).astype(kind)


def setup_inputs(seed: int = 0) -> dict:
    splits = jax.random.split(jax.random.key(seed), 8)
    query_states = draw_query_states(jax.random.fold_in(splits[7], 71), 0)
    key_states = draw_key_states(jax.random.fold_in(splits[7], 71), 0)
    value_states = normal_values(splits[2], (SEQS, LEN, HD), 1.0, 6.0, ((0, 4), (1, 8)))
    span_order = draw_span_order(jax.random.fold_in(splits[7], 71), 0)
    block_mask = draw_block_mask(jax.random.fold_in(splits[7], 71), 0)
    output_weight = normal_values(splits[5], (HD, D), HD ** -0.5, 0.1875, ((0, 32),))
    upstream = normal_values(splits[6], (SEQS, LEN, D), 1.0, 6.0, ((0, 4), (1, 8)))
    return {"query_states": query_states, "key_states": key_states, "value_states": value_states, "span_order": span_order, "block_mask": block_mask, "output_weight": output_weight, "upstream": upstream}


def reference(query_states, key_states, value_states, span_order, block_mask, output_weight, upstream):
    span_rows = CH
    positions = (span_order[:, None] * span_rows + jnp.arange(span_rows, dtype=jnp.int32)[None, :]).reshape(-1)
    onehot = (span_order[:, None] == jnp.arange(NCH, dtype=jnp.int32)[None, :]).astype(jnp.float32)
    span_ok = jnp.dot(jnp.dot(onehot, block_mask.astype(jnp.float32)), onehot.T) > 0.5
    row_span = jnp.arange(LEN, dtype=jnp.int32) // span_rows
    score_scale = 1.0 / HEAD

    def one_sequence(arrays):
        queries, key_all, value_all, grad_all = arrays
        key_f32 = key_all.astype(jnp.float32).reshape(LEN, HEADS, HEAD)
        value_f32 = value_all.astype(jnp.float32).reshape(LEN, HEADS, HEAD)

        def block_step(carry, step_index):
            key_sum, value_sum, weight_sum = carry
            begin_row = step_index * TOK_DEV
            query_block = lax.dynamic_slice_in_dim(queries, begin_row, TOK_DEV)
            grad_rows = lax.dynamic_slice_in_dim(grad_all, begin_row, TOK_DEV)
            query_pos = lax.dynamic_slice_in_dim(positions, begin_row, TOK_DEV)
            query_span = lax.dynamic_slice_in_dim(row_span, begin_row, TOK_DEV)
            allowed = span_ok[query_span][:, row_span] & (positions[None, :] <= query_pos[:, None])
            query_f32 = query_block.astype(jnp.float32).reshape(TOK_DEV, HEADS, HEAD)
            scores = jnp.einsum('qhd,khd->hqk', query_f32, key_f32) * score_scale
            masked = jnp.where(allowed[None], scores, -jnp.inf)
            row_max = masked.max(-1)
            exp_terms = jnp.where(allowed[None], jnp.exp(scores - row_max[..., None]), 0.0)
            log_total = row_max + jnp.log(exp_terms.sum(-1))
            probability = jnp.where(allowed[None], jnp.exp(scores - log_total[..., None]), 0.0)
            probability_low = lax.optimization_barrier(probability.astype(jnp.bfloat16))
            attended = jnp.einsum('hqk,khd->qhd', probability_low.astype(jnp.float32), value_f32)
            attended = lax.optimization_barrier(attended.reshape(TOK_DEV, HD).astype(jnp.bfloat16))
            projected = jnp.dot(attended, output_weight, preferred_element_type=jnp.float32).astype(jnp.bfloat16)
            grad_attended = jnp.dot(grad_rows, output_weight.T, preferred_element_type=jnp.float32).astype(jnp.bfloat16)
            grad_attended = lax.optimization_barrier(grad_attended)
            grad_f32 = grad_attended.astype(jnp.float32).reshape(TOK_DEV, HEADS, HEAD)
            row_delta = (grad_f32 * attended.astype(jnp.float32).reshape(TOK_DEV, HEADS, HEAD)).sum(-1)
            dprob = jnp.einsum('qhd,khd->hqk', grad_f32, value_f32)
            dscores = (probability * (dprob - row_delta.T[..., None]) * score_scale).astype(jnp.bfloat16)
            dscores_f32 = lax.optimization_barrier(dscores).astype(jnp.float32)
            query_grad = jnp.einsum('hqk,khd->qhd', dscores_f32, key_f32).reshape(TOK_DEV, HD).astype(jnp.bfloat16)
            key_piece = jnp.einsum('hqk,qhd->khd', dscores_f32, query_f32).astype(jnp.bfloat16)
            value_piece = jnp.einsum('hqk,qhd->khd', probability_low.astype(jnp.float32), grad_f32).astype(jnp.bfloat16)
            weight_piece = jnp.dot(attended.T, grad_rows, preferred_element_type=jnp.float32).astype(jnp.bfloat16)
            key_piece, value_piece, weight_piece = lax.optimization_barrier((key_piece, value_piece, weight_piece))
            updated = (key_sum + key_piece.astype(jnp.float32), value_sum + value_piece.astype(jnp.float32),
                       weight_sum + weight_piece.astype(jnp.float32))
            return updated, (projected, query_grad)

        start_sums = (jnp.zeros((LEN, HEADS, HEAD), jnp.float32), jnp.zeros((LEN, HEADS, HEAD), jnp.float32),
                      jnp.zeros((HD, D), jnp.float32))
        sums_out, rows_out = lax.scan(block_step, start_sums, jnp.arange(N_CP, dtype=jnp.int32))
        key_sum, value_sum, weight_sum = sums_out
        projected, query_grad = rows_out
        return (projected.reshape(LEN, D), query_grad.reshape(LEN, HD),
                key_sum.reshape(LEN, HD).astype(jnp.bfloat16), value_sum.reshape(LEN, HD).astype(jnp.bfloat16),
                weight_sum)

    projected, query_gradient, key_gradient, value_gradient, weight_sums = lax.map(
        one_sequence, (query_states, key_states, value_states, upstream))
    return projected, query_gradient, key_gradient, value_gradient, weight_sums.sum(0)
```

```python
import math

import jax
import jax.numpy as jnp
from jax import lax
from jax.experimental import pallas as pl
from jax.experimental.pallas import tpu as pltpu
from jax.sharding import PartitionSpec as P

HEADS = 8
HEAD = 128


lowest = -1e30


def split_heads(row_block):
    return row_block.reshape(row_block.shape[0], HEADS, HEAD)


def pair_scores(query_rows, key_rows):
    return jnp.einsum(
        "qhd,khd->hqk",
        split_heads(query_rows),
        split_heads(key_rows),
        preferred_element_type=jnp.float32,
    ) * (1.0 / HEAD)


def storage_mask(span_order, block_mask):
    span_count = span_order.shape[0]
    onehot = (span_order[:, None] == jnp.arange(span_count, dtype=jnp.int32)[None, :]).astype(
        jnp.float32
    )
    permuted = jnp.dot(jnp.dot(onehot, block_mask.astype(jnp.float32)), onehot.T)
    return permuted > 0.5


def allowed_block(span_ok, positions, query_begin, query_total, key_begin, key_total, span_rows):
    span_sub = lax.dynamic_slice(
        span_ok,
        (query_begin // span_rows, key_begin // span_rows),
        (query_total // span_rows, key_total // span_rows),
    )
    spread = jnp.broadcast_to(
        span_sub[:, None, :, None],
        (query_total // span_rows, span_rows, key_total // span_rows, span_rows),
    )
    spread = spread.reshape(query_total, key_total)
    query_pos = lax.dynamic_slice_in_dim(positions, query_begin, query_total)
    key_pos = lax.dynamic_slice_in_dim(positions, key_begin, key_total)
    return spread & (key_pos[None, :] <= query_pos[:, None])


def local_terms(query_rows, grad_rows, log_rows, delta_rows, key_rows, value_rows, allowed):
    scores = pair_scores(query_rows, key_rows)
    probability = jnp.where(allowed[None], jnp.exp(scores - log_rows[..., None]), 0.0)
    dprob = jnp.einsum(
        "qhd,khd->hqk",
        split_heads(grad_rows),
        split_heads(value_rows),
        preferred_element_type=jnp.float32,
    )
    dscores = (probability * (dprob - delta_rows[..., None]) * (1.0 / HEAD)).astype(jnp.bfloat16)
    return (probability, dscores)


def local(query_states, key_states, value_states, span_order, block_mask, output_weight, upstream):
    query_rows = query_states[0]
    key_local = key_states[0]
    value_local = value_states[0]
    upstream_rows = upstream[0]
    tokens = query_rows.shape[0]
    span_rows = tokens // 2
    positions = (
        span_order[:, None] * span_rows + jnp.arange(span_rows, dtype=jnp.int32)[None, :]
    ).reshape(-1)
    span_ok = storage_mask(span_order, block_mask)
    own_start = lax.axis_index("cp") * tokens
    key_all, value_all = (
        lax.all_gather(key_local, "cp", axis=0, tiled=True),
        lax.all_gather(value_local, "cp", axis=0, tiled=True),
    )
    weight = lax.all_gather(output_weight, ("cp", "fsdp"), axis=0, tiled=True)
    length = key_all.shape[0]
    key_block = math.gcd(length, 512)
    block_count = length // key_block
    block_steps = jnp.arange(block_count, dtype=jnp.int32)

    def stats_step(running, step_index):
        key_begin = step_index * key_block
        key_rows = lax.dynamic_slice_in_dim(key_all, key_begin, key_block)
        allowed = allowed_block(
            span_ok, positions, own_start, tokens, key_begin, key_block, span_rows
        )
        maxima, totals = running
        scores = pair_scores(query_rows, key_rows)
        masked = jnp.where(allowed[None], scores, lowest)
        new_max = jnp.maximum(maxima, masked.max(-1))
        exp_terms = jnp.where(allowed[None], jnp.exp(scores - new_max[..., None]), 0.0)
        return ((new_max, totals * jnp.exp(maxima - new_max) + exp_terms.sum(-1)), None)

    stat_start = (
        jnp.full((HEADS, tokens), lowest, jnp.float32),
        jnp.zeros((HEADS, tokens), jnp.float32),
    )
    (maxima, totals), _ = lax.scan(stats_step, stat_start, block_steps)
    log_total = maxima + jnp.log(totals)

    def output_step(attn_sum, step_index):
        key_begin = step_index * key_block
        key_rows = lax.dynamic_slice_in_dim(key_all, key_begin, key_block)
        value_rows = lax.dynamic_slice_in_dim(value_all, key_begin, key_block)
        allowed = allowed_block(
            span_ok, positions, own_start, tokens, key_begin, key_block, span_rows
        )
        scores = pair_scores(query_rows, key_rows)
        probability = jnp.where(allowed[None], jnp.exp(scores - log_total[..., None]), 0.0)
        return (
            attn_sum
            + jnp.einsum(
                "hqk,khd->qhd",
                probability.astype(jnp.bfloat16),
                split_heads(value_rows),
                preferred_element_type=jnp.float32,
            ),
            None,
        )

    zero_heads = jnp.zeros((tokens, HEADS, HEAD), jnp.float32)
    attn_sum, _ = lax.scan(output_step, zero_heads, block_steps)
    attended = lax.optimization_barrier(attn_sum.reshape(tokens, -1).astype(jnp.bfloat16))
    projected = jnp.dot(attended, weight, preferred_element_type=jnp.float32).astype(jnp.bfloat16)
    grad_attended = lax.dot_general(
        upstream_rows, weight, (((1,), (1,)), ((), ())), preferred_element_type=jnp.float32
    ).astype(jnp.bfloat16)
    grad_attended = lax.optimization_barrier(grad_attended)
    weight_term = lax.dot_general(
        attended, upstream_rows, (((0,), (0,)), ((), ())), preferred_element_type=jnp.float32
    )
    row_delta = (
        (grad_attended.astype(jnp.float32) * attended.astype(jnp.float32))
        .reshape(tokens, HEADS, HEAD)
        .sum(-1)
    )
    delta_heads = row_delta.T

    def query_step(grad_sum, step_index):
        key_begin = step_index * key_block
        key_rows = lax.dynamic_slice_in_dim(key_all, key_begin, key_block)
        value_rows = lax.dynamic_slice_in_dim(value_all, key_begin, key_block)
        allowed = allowed_block(
            span_ok, positions, own_start, tokens, key_begin, key_block, span_rows
        )
        probability, dscores = local_terms(
            query_rows, grad_attended, log_total, delta_heads, key_rows, value_rows, allowed
        )
        return (
            grad_sum
            + jnp.einsum(
                "hqk,khd->qhd", dscores, split_heads(key_rows), preferred_element_type=jnp.float32
            ),
            None,
        )

    query_sum, _ = lax.scan(query_step, zero_heads, block_steps)
    query_gradient = query_sum.reshape(tokens, -1).astype(jnp.bfloat16)
    log_all, delta_all = (
        lax.all_gather(log_total.T, "cp", axis=0, tiled=True),
        lax.all_gather(row_delta, "cp", axis=0, tiled=True),
    )
    sums_now = (zero_heads, zero_heads)
    query_piece = lax.all_gather(query_rows, "cp", axis=0, tiled=True)
    grad_piece = lax.all_gather(grad_attended, "cp", axis=0, tiled=True)
    row_count = query_piece.shape[0]
    sources = row_count // tokens
    group_size = math.gcd(sources, max(1, 512 // tokens))
    group_rows = group_size * tokens

    def group_step(running, step_index):
        offset = step_index * group_rows
        query_group = lax.dynamic_slice_in_dim(query_piece, offset, group_rows)
        grad_group = lax.dynamic_slice_in_dim(grad_piece, offset, group_rows)
        log_group = lax.dynamic_slice_in_dim(log_all, offset, group_rows).T
        delta_group = lax.dynamic_slice_in_dim(delta_all, offset, group_rows).T
        allowed = allowed_block(
            span_ok, positions, offset, group_rows, own_start, tokens, span_rows
        )
        key_sum, value_sum = running
        probability, dscores = local_terms(
            query_group, grad_group, log_group, delta_group, key_local, value_local, allowed
        )
        probability_low = probability.astype(jnp.bfloat16).reshape(
            HEADS, group_size, tokens, tokens
        )
        dscores_group = dscores.reshape(HEADS, group_size, tokens, tokens)
        qsplit = query_group.reshape(group_size, tokens, HEADS, HEAD)
        gsplit = grad_group.reshape(group_size, tokens, HEADS, HEAD)
        key_part = jnp.einsum(
            "hgqk,gqhd->gkhd", dscores_group, qsplit, preferred_element_type=jnp.float32
        ).astype(jnp.bfloat16)
        value_part = jnp.einsum(
            "hgqk,gqhd->gkhd", probability_low, gsplit, preferred_element_type=jnp.float32
        ).astype(jnp.bfloat16)
        key_part, value_part = lax.optimization_barrier((key_part, value_part))
        return (
            (
                key_sum + key_part.astype(jnp.float32).sum(0),
                value_sum + value_part.astype(jnp.float32).sum(0),
            ),
            None,
        )

    sums_now, _ = lax.scan(group_step, sums_now, jnp.arange(sources // group_size, dtype=jnp.int32))
    key_sum, value_sum = sums_now
    key_gradient = key_sum.reshape(tokens, -1).astype(jnp.bfloat16)
    value_gradient = value_sum.reshape(tokens, -1).astype(jnp.bfloat16)
    cycle_count = lax.axis_size("cp")
    batch_count = lax.axis_size("fsdp")
    slab_rows = weight_term.shape[0] // (cycle_count * batch_count)
    reordered = weight_term.reshape(cycle_count, batch_count, slab_rows, -1).transpose(1, 0, 2, 3)
    reordered = reordered.reshape(weight_term.shape[0], -1)
    partial_batch = lax.psum_scatter(
        reordered.astype(jnp.bfloat16), "fsdp", scatter_dimension=0, tiled=True
    )
    weight_gradient = lax.psum_scatter(partial_batch, "cp", scatter_dimension=0, tiled=True).astype(
        jnp.float32
    )
    return (
        projected[None],
        query_gradient[None],
        key_gradient[None],
        value_gradient[None],
        weight_gradient,
    )


MESH = pl.DeviceIdType.MESH


def remote(src, dst, send_sem, recv_sem, device):
    return pltpu.make_async_remote_copy(
        src_ref=src,
        dst_ref=dst,
        send_sem=send_sem,
        recv_sem=recv_sem,
        device_id=device,
        device_id_type=MESH,
    )


def rows_of(begin, count):
    return pl.ds(pl.multiple_of(begin, count), count)


def greet(devices):
    barrier = pltpu.get_barrier_semaphore()
    for device in devices:
        pl.semaphore_signal(barrier, inc=1, device_id=device, device_id_type=MESH)
    pl.semaphore_wait(barrier, len(devices))


def gather_kernel(
    n, q, k, v, up, w, qh, kh, vh, ups, wall,
    local_sem, heads_s, heads_r, ring_s, ring_r, part_s, part_r, cross_s, cross_r, relay_s, relay_r,
):
    me = lax.axis_index("cp")
    col = lax.axis_index("fsdp")
    partner = {"fsdp": col + 1 - 2 * lax.rem(col, 2)}
    cross_col = lax.rem(col + 2, 4)
    cross = {"fsdp": cross_col}
    tokens = up.shape[0]
    half = tokens // 2
    slab = w.shape[0]
    depth = n // 2
    zed, why = me // 2, lax.rem(me, 2)
    place = zed + why * (n - 1 - 2 * zed)

    def at_place(offset):
        r = lax.rem(place + offset + 2 * n, n)
        return 2 * r + (r // depth) * (2 * n - 1 - 4 * r)

    def head_cols(d):
        return rows_of(d * HEAD, HEAD)

    peers = [{"cp": lax.rem(me + i, n)} for i in range(1, n)]
    greet(peers + [partner, cross])

    def chunk_ref(which, owner):
        if which == 2:
            return wall.at[rows_of(owner * (4 * slab) + col * slab, slab)]
        return ups.at[rows_of(owner * tokens + which * half, half)]

    def own_ref(which):
        if which == 2:
            return w
        return up.at[rows_of(which * half, half)]

    sends = []
    toward = ({"cp": at_place(1)}, {"cp": at_place(-1)})

    def chunks_at(step, way):
        if step < depth:
            return (2, 0, 1)
        return (2, 0) if way == 0 else (1,)

    def ring_start(step, way, which):
        owner = at_place((1 - step) if way == 0 else (step - 1))
        source = own_ref(which) if step == 1 else chunk_ref(which, owner)
        copy = remote(
            source, chunk_ref(which, owner),
            ring_s.at[way, step, which], ring_r.at[way, step, which], toward[way],
        )
        copy.start()
        sends.append(copy)

    def ring_wait(step, way, which):
        owner = at_place(-step if way == 0 else step)
        block = chunk_ref(which, owner)
        remote(
            block, block, ring_s.at[way, step, which], ring_r.at[way, step, which], toward[way]
        ).wait_recv()

    spread = []

    def spread_weight(owner, source):
        slot = len(spread)
        spread.append(owner)
        block = chunk_ref(2, owner)
        for device, ss, rs in ((cross, cross_s, cross_r), (partner, part_s, part_r)):
            copy = remote(source, block, ss.at[slot], rs.at[slot], device)
            copy.start()
            sends.append(copy)

    for way in range(2):
        for which in chunks_at(1, way):
            ring_start(1, way, which)
    triples = ((q, qh), (k, kh), (v, vh))
    for i in range(1, n):
        d = lax.rem(me + i, n)
        for t, (a, b) in enumerate(triples):
            copy = remote(
                a.at[:, head_cols(d)], b.at[rows_of(me * tokens, tokens)],
                heads_s.at[t, i], heads_r.at[t, i], {"cp": d},
            )
            copy.start()
            sends.append(copy)
    own = [
        pltpu.make_async_copy(
            a.at[:, head_cols(me)], b.at[rows_of(me * tokens, tokens)], local_sem.at[t]
        )
        for t, (a, b) in enumerate(triples)
    ]
    own.append(pltpu.make_async_copy(up, ups.at[rows_of(me * tokens, tokens)], local_sem.at[3]))
    own.append(pltpu.make_async_copy(w, chunk_ref(2, me), local_sem.at[4]))
    for copy in own:
        copy.start()
    spread_weight(me, w)
    for step in range(1, depth + 1):
        for way in range(2):
            for which in chunks_at(step, way):
                ring_wait(step, way, which)
                if step < depth and which in chunks_at(step + 1, way):
                    ring_start(step + 1, way, which)
                if which == 2:
                    owner = at_place(-step if way == 0 else step)
                    spread_weight(owner, chunk_ref(2, owner))
    for slot, owner in enumerate(spread):
        block = wall.at[rows_of(owner * (4 * slab) + cross_col * slab, slab)]
        remote(block, block, cross_s.at[slot], cross_r.at[slot], cross).wait_recv()
        copy = remote(block, block, relay_s.at[slot], relay_r.at[slot], partner)
        copy.start()
        sends.append(copy)
    for i in range(1, n):
        source = lax.rem(me + n - i, n)
        for t, (a, b) in enumerate(triples):
            block = b.at[rows_of(source * tokens, tokens)]
            remote(block, block, heads_s.at[t, i], heads_r.at[t, i], {"cp": source}).wait_recv()
    near = partner["fsdp"]
    far = lax.rem(near + 2, 4)
    for slot, owner in enumerate(spread):
        for other, ss, rs in ((near, part_s, part_r), (far, relay_s, relay_r)):
            block = wall.at[rows_of(owner * (4 * slab) + other * slab, slab)]
            remote(block, block, ss.at[slot], rs.at[slot], partner).wait_recv()
    for copy in own:
        copy.wait()
    for copy in sends:
        copy.wait_send()


def scatter_kernel(n, m, a0, a1, a2, a3, dw, b0, b1, b2, b3, dwr, local_sem, ss, rs, ws, wr):
    me = lax.axis_index("cp")
    col = lax.axis_index("fsdp")
    tokens = b0.shape[0]
    slab = dwr.shape[1]
    pairs = ((a0, b0), (a1, b1), (a2, b2), (a3, b3))
    peers = [{"cp": lax.rem(me + i, n)} for i in range(1, n)]
    columns = [{"fsdp": lax.rem(col + j, m)} for j in range(1, m)]
    greet(peers + columns)
    sends = []
    for t, (a, b) in enumerate(pairs):
        for i in range(1, n):
            d = lax.rem(me + i, n)
            copy = remote(
                a.at[rows_of(d * tokens, tokens)], b.at[:, rows_of(me * HEAD, HEAD)],
                ss.at[t, i], rs.at[t, i], {"cp": d},
            )
            copy.start()
            sends.append(copy)
    for j in range(1, m):
        g = lax.rem(col + j, m)
        copy = remote(
            dw.at[rows_of(g * slab, slab)], dwr.at[j], ws.at[j], wr.at[j], {"fsdp": g}
        )
        copy.start()
        sends.append(copy)
    own = [
        pltpu.make_async_copy(
            a.at[rows_of(me * tokens, tokens)], b.at[:, rows_of(me * HEAD, HEAD)], local_sem.at[t]
        )
        for t, (a, b) in enumerate(pairs)
    ]
    own.append(
        pltpu.make_async_copy(dw.at[rows_of(col * slab, slab)], dwr.at[0], local_sem.at[4])
    )
    for copy in own:
        copy.start()
    for t, (a, b) in enumerate(pairs):
        for i in range(1, n):
            source = lax.rem(me + n - i, n)
            block = b.at[:, rows_of(source * HEAD, HEAD)]
            remote(block, block, ss.at[t, i], rs.at[t, i], {"cp": source}).wait_recv()
    for j in range(1, m):
        block = dwr.at[j]
        remote(block, block, ws.at[j], wr.at[j], columns[j - 1]).wait_recv()
    for copy in own:
        copy.wait()
    for copy in sends:
        copy.wait_send()


def attention_kernel(q, k, v, ga, allowed, att, dq, dk, dv, kt, vt, dk_sum, dv_sum):
    step = pl.program_id(0)

    @pl.when(step == 0)
    def _():
        kt[...] = k[...].astype(jnp.float32).T.astype(jnp.bfloat16)
        vt[...] = v[...].astype(jnp.float32).T.astype(jnp.bfloat16)
        dk_sum[...] = jnp.zeros_like(dk_sum)
        dv_sum[...] = jnp.zeros_like(dv_sum)

    f32 = jnp.float32
    nt = (((1,), (1,)), ((), ()))
    scores = lax.dot_general(k[...], q[...], nt, preferred_element_type=f32) * (1.0 / HEAD)
    scores = jnp.where(allowed[...].astype(f32) > 0.5, scores, lowest)
    top = scores.max(0, keepdims=True)
    terms = jnp.exp(scores - top)
    probability = terms * (1.0 / terms.sum(0, keepdims=True))
    low = probability.astype(jnp.bfloat16)
    att_t = jnp.dot(vt[...], low, preferred_element_type=f32).astype(jnp.bfloat16).astype(f32)
    att[...] = att_t.T.astype(jnp.bfloat16)
    delta = (att_t * ga[...].astype(f32).T).sum(0, keepdims=True)
    dprob = lax.dot_general(v[...], ga[...], nt, preferred_element_type=f32)
    ds = (probability * (dprob - delta) * (1.0 / HEAD)).astype(jnp.bfloat16)
    dq_t = jnp.dot(kt[...], ds, preferred_element_type=f32)
    dq[...] = dq_t.T.astype(jnp.bfloat16)
    dk_sum[...] += jnp.dot(ds, q[...], preferred_element_type=f32)
    dv_sum[...] += jnp.dot(low, ga[...], preferred_element_type=f32)

    @pl.when(step == pl.num_programs(0) - 1)
    def _():
        dk[...] = dk_sum[...].astype(jnp.bfloat16)
        dv[...] = dv_sum[...].astype(jnp.bfloat16)


def by_heads(query_states, key_states, value_states, span_order, block_mask, output_weight, upstream):
    n = lax.axis_size("cp")
    m = lax.axis_size("fsdp")
    tokens, width = query_states.shape[1:]
    length = tokens * n
    model = upstream.shape[2]
    slab = output_weight.shape[0]
    span_rows = tokens // 2
    bf16 = jnp.bfloat16
    shape = jax.ShapeDtypeStruct
    vmem = pl.BlockSpec(memory_space=pltpu.VMEM)
    anywhere = pl.BlockSpec(memory_space=pl.ANY)
    dma = pltpu.SemaphoreType.DMA
    half = n // 2
    qh, kh, vh, ups, weight = pl.pallas_call(
        lambda *refs: gather_kernel(n, *refs),
        out_shape=(shape((length, HEAD), bf16),) * 3
        + (shape((length, model), bf16), shape((width, model), bf16)),
        in_specs=[vmem] * 5,
        out_specs=(anywhere,) * 5,
        scratch_shapes=[
            dma((5,)), dma((3, n)), dma((3, n)), dma((2, half + 1, 3)), dma((2, half + 1, 3)),
        ]
        + [dma((n,))] * 6,
        compiler_params=pltpu.CompilerParams(collective_id=0, has_side_effects=True),
        name="gather",
    )(query_states[0], key_states[0], value_states[0], upstream[0], output_weight)
    head_rows = lax.dynamic_slice_in_dim(weight, lax.axis_index("cp") * HEAD, HEAD)
    ga = lax.dot_general(
        ups, head_rows, (((1,), (1,)), ((), ())), preferred_element_type=jnp.float32
    ).astype(bf16)
    positions = (
        span_order[:, None] * span_rows + jnp.arange(span_rows, dtype=jnp.int32)[None, :]
    ).reshape(-1)
    span_ok = storage_mask(span_order, block_mask)
    allowed = allowed_block(span_ok, positions, 0, length, 0, length, span_rows)
    allowed = allowed.T.astype(bf16)
    block = math.gcd(length, 256)
    rows = pl.BlockSpec((block, HEAD), lambda i: (i, 0))
    whole = pl.BlockSpec((length, HEAD), lambda i: (0, 0))
    att_h, dq_h, dk_h, dv_h = pl.pallas_call(
        attention_kernel,
        grid=(length // block,),
        out_shape=(shape((length, HEAD), bf16),) * 4,
        in_specs=[rows, whole, whole, rows, pl.BlockSpec((length, block), lambda i: (0, i))],
        out_specs=(rows, rows, whole, whole),
        scratch_shapes=[pltpu.VMEM((HEAD, length), bf16)] * 2
        + [pltpu.VMEM((length, HEAD), jnp.float32)] * 2,
        compiler_params=pltpu.CompilerParams(dimension_semantics=("arbitrary",)),
        name="attention",
    )(qh, kh, vh, ga, allowed)
    weight_term = lax.dot_general(
        att_h, ups, (((0,), (0,)), ((), ())), preferred_element_type=jnp.float32
    ).astype(bf16)
    attended, dq, dk, dv, pieces = pl.pallas_call(
        lambda *refs: scatter_kernel(n, m, *refs),
        out_shape=(shape((tokens, width), bf16),) * 4 + (shape((m, slab, model), bf16),),
        in_specs=[vmem] * 5,
        out_specs=(vmem,) * 5,
        scratch_shapes=[dma((5,)), dma((4, n)), dma((4, n)), dma((m,)), dma((m,))],
        compiler_params=pltpu.CompilerParams(collective_id=1, has_side_effects=True),
        name="scatter",
    )(att_h, dq_h, dk_h, dv_h, weight_term)
    projected = jnp.dot(attended, weight, preferred_element_type=jnp.float32).astype(bf16)
    weight_gradient = pieces.astype(jnp.float32).sum(0)
    return (projected[None], dq[None], dk[None], dv[None], weight_gradient)


def solution(mesh):
    fits = mesh.shape["cp"] == HEADS and mesh.shape["fsdp"] == 4
    return jax.shard_map(
        by_heads if fits else local,
        mesh=mesh,
        in_specs=(
            P("fsdp", "cp", None),
            P("fsdp", "cp", None),
            P("fsdp", "cp", None),
            P(),
            P(),
            P(("cp", "fsdp"), None),
            P("fsdp", "cp", None),
        ),
        out_specs=(
            P("fsdp", "cp", None),
            P("fsdp", "cp", None),
            P("fsdp", "cp", None),
            P("fsdp", "cp", None),
            P(("cp", "fsdp"), None),
        ),
        check_vma=False,
    )
```

```python
import math

import jax
import jax.numpy as jnp
from jax import lax
from jax.experimental import pallas as pl
from jax.experimental.pallas import tpu as pltpu
from jax.sharding import PartitionSpec as P

HEADS = 8
HEAD = 128


lowest = -1e30


def split_heads(row_block):
    return row_block.reshape(row_block.shape[0], HEADS, HEAD)


def pair_scores(query_rows, key_rows):
    return jnp.einsum(
        "qhd,khd->hqk",
        split_heads(query_rows),
        split_heads(key_rows),
        preferred_element_type=jnp.float32,
    ) * (1.0 / HEAD)


def storage_mask(span_order, block_mask):
    span_count = span_order.shape[0]
    onehot = (span_order[:, None] == jnp.arange(span_count, dtype=jnp.int32)[None, :]).astype(
        jnp.float32
    )
    permuted = jnp.dot(jnp.dot(onehot, block_mask.astype(jnp.float32)), onehot.T)
    return permuted > 0.5


def allowed_block(span_ok, positions, query_begin, query_total, key_begin, key_total, span_rows):
    span_sub = lax.dynamic_slice(
        span_ok,
        (query_begin // span_rows, key_begin // span_rows),
        (query_total // span_rows, key_total // span_rows),
    )
    spread = jnp.broadcast_to(
        span_sub[:, None, :, None],
        (query_total // span_rows, span_rows, key_total // span_rows, span_rows),
    )
    spread = spread.reshape(query_total, key_total)
    query_pos = lax.dynamic_slice_in_dim(positions, query_begin, query_total)
    key_pos = lax.dynamic_slice_in_dim(positions, key_begin, key_total)
    return spread & (key_pos[None, :] <= query_pos[:, None])


def local_terms(query_rows, grad_rows, log_rows, delta_rows, key_rows, value_rows, allowed):
    scores = pair_scores(query_rows, key_rows)
    probability = jnp.where(allowed[None], jnp.exp(scores - log_rows[..., None]), 0.0)
    dprob = jnp.einsum(
        "qhd,khd->hqk",
        split_heads(grad_rows),
        split_heads(value_rows),
        preferred_element_type=jnp.float32,
    )
    dscores = (probability * (dprob - delta_rows[..., None]) * (1.0 / HEAD)).astype(jnp.bfloat16)
    return (probability, dscores)


def local(query_states, key_states, value_states, span_order, block_mask, output_weight, upstream):
    query_rows = query_states[0]
    key_local = key_states[0]
    value_local = value_states[0]
    upstream_rows = upstream[0]
    tokens = query_rows.shape[0]
    span_rows = tokens // 2
    positions = (
        span_order[:, None] * span_rows + jnp.arange(span_rows, dtype=jnp.int32)[None, :]
    ).reshape(-1)
    span_ok = storage_mask(span_order, block_mask)
    own_start = lax.axis_index("cp") * tokens
    key_all, value_all = (
        lax.all_gather(key_local, "cp", axis=0, tiled=True),
        lax.all_gather(value_local, "cp", axis=0, tiled=True),
    )
    weight = lax.all_gather(output_weight, ("cp", "fsdp"), axis=0, tiled=True)
    length = key_all.shape[0]
    key_block = math.gcd(length, 512)
    block_count = length // key_block
    block_steps = jnp.arange(block_count, dtype=jnp.int32)

    def stats_step(running, step_index):
        key_begin = step_index * key_block
        key_rows = lax.dynamic_slice_in_dim(key_all, key_begin, key_block)
        allowed = allowed_block(
            span_ok, positions, own_start, tokens, key_begin, key_block, span_rows
        )
        maxima, totals = running
        scores = pair_scores(query_rows, key_rows)
        masked = jnp.where(allowed[None], scores, lowest)
        new_max = jnp.maximum(maxima, masked.max(-1))
        exp_terms = jnp.where(allowed[None], jnp.exp(scores - new_max[..., None]), 0.0)
        return ((new_max, totals * jnp.exp(maxima - new_max) + exp_terms.sum(-1)), None)

    stat_start = (
        jnp.full((HEADS, tokens), lowest, jnp.float32),
        jnp.zeros((HEADS, tokens), jnp.float32),
    )
    (maxima, totals), _ = lax.scan(stats_step, stat_start, block_steps)
    log_total = maxima + jnp.log(totals)

    def output_step(attn_sum, step_index):
        key_begin = step_index * key_block
        key_rows = lax.dynamic_slice_in_dim(key_all, key_begin, key_block)
        value_rows = lax.dynamic_slice_in_dim(value_all, key_begin, key_block)
        allowed = allowed_block(
            span_ok, positions, own_start, tokens, key_begin, key_block, span_rows
        )
        scores = pair_scores(query_rows, key_rows)
        probability = jnp.where(allowed[None], jnp.exp(scores - log_total[..., None]), 0.0)
        return (
            attn_sum
            + jnp.einsum(
                "hqk,khd->qhd",
                probability.astype(jnp.bfloat16),
                split_heads(value_rows),
                preferred_element_type=jnp.float32,
            ),
            None,
        )

    zero_heads = jnp.zeros((tokens, HEADS, HEAD), jnp.float32)
    attn_sum, _ = lax.scan(output_step, zero_heads, block_steps)
    attended = lax.optimization_barrier(attn_sum.reshape(tokens, -1).astype(jnp.bfloat16))
    projected = jnp.dot(attended, weight, preferred_element_type=jnp.float32).astype(jnp.bfloat16)
    grad_attended = lax.dot_general(
        upstream_rows, weight, (((1,), (1,)), ((), ())), preferred_element_type=jnp.float32
    ).astype(jnp.bfloat16)
    grad_attended = lax.optimization_barrier(grad_attended)
    weight_term = lax.dot_general(
        attended, upstream_rows, (((0,), (0,)), ((), ())), preferred_element_type=jnp.float32
    )
    row_delta = (
        (grad_attended.astype(jnp.float32) * attended.astype(jnp.float32))
        .reshape(tokens, HEADS, HEAD)
        .sum(-1)
    )
    delta_heads = row_delta.T

    def query_step(grad_sum, step_index):
        key_begin = step_index * key_block
        key_rows = lax.dynamic_slice_in_dim(key_all, key_begin, key_block)
        value_rows = lax.dynamic_slice_in_dim(value_all, key_begin, key_block)
        allowed = allowed_block(
            span_ok, positions, own_start, tokens, key_begin, key_block, span_rows
        )
        probability, dscores = local_terms(
            query_rows, grad_attended, log_total, delta_heads, key_rows, value_rows, allowed
        )
        return (
            grad_sum
            + jnp.einsum(
                "hqk,khd->qhd", dscores, split_heads(key_rows), preferred_element_type=jnp.float32
            ),
            None,
        )

    query_sum, _ = lax.scan(query_step, zero_heads, block_steps)
    query_gradient = query_sum.reshape(tokens, -1).astype(jnp.bfloat16)
    log_all, delta_all = (
        lax.all_gather(log_total.T, "cp", axis=0, tiled=True),
        lax.all_gather(row_delta, "cp", axis=0, tiled=True),
    )
    sums_now = (zero_heads, zero_heads)
    query_piece = lax.all_gather(query_rows, "cp", axis=0, tiled=True)
    grad_piece = lax.all_gather(grad_attended, "cp", axis=0, tiled=True)
    row_count = query_piece.shape[0]
    sources = row_count // tokens
    group_size = math.gcd(sources, max(1, 512 // tokens))
    group_rows = group_size * tokens

    def group_step(running, step_index):
        offset = step_index * group_rows
        query_group = lax.dynamic_slice_in_dim(query_piece, offset, group_rows)
        grad_group = lax.dynamic_slice_in_dim(grad_piece, offset, group_rows)
        log_group = lax.dynamic_slice_in_dim(log_all, offset, group_rows).T
        delta_group = lax.dynamic_slice_in_dim(delta_all, offset, group_rows).T
        allowed = allowed_block(
            span_ok, positions, offset, group_rows, own_start, tokens, span_rows
        )
        key_sum, value_sum = running
        probability, dscores = local_terms(
            query_group, grad_group, log_group, delta_group, key_local, value_local, allowed
        )
        probability_low = probability.astype(jnp.bfloat16).reshape(
            HEADS, group_size, tokens, tokens
        )
        dscores_group = dscores.reshape(HEADS, group_size, tokens, tokens)
        qsplit = query_group.reshape(group_size, tokens, HEADS, HEAD)
        gsplit = grad_group.reshape(group_size, tokens, HEADS, HEAD)
        key_part = jnp.einsum(
            "hgqk,gqhd->gkhd", dscores_group, qsplit, preferred_element_type=jnp.float32
        ).astype(jnp.bfloat16)
        value_part = jnp.einsum(
            "hgqk,gqhd->gkhd", probability_low, gsplit, preferred_element_type=jnp.float32
        ).astype(jnp.bfloat16)
        key_part, value_part = lax.optimization_barrier((key_part, value_part))
        return (
            (
                key_sum + key_part.astype(jnp.float32).sum(0),
                value_sum + value_part.astype(jnp.float32).sum(0),
            ),
            None,
        )

    sums_now, _ = lax.scan(group_step, sums_now, jnp.arange(sources // group_size, dtype=jnp.int32))
    key_sum, value_sum = sums_now
    key_gradient = key_sum.reshape(tokens, -1).astype(jnp.bfloat16)
    value_gradient = value_sum.reshape(tokens, -1).astype(jnp.bfloat16)
    cycle_count = lax.axis_size("cp")
    batch_count = lax.axis_size("fsdp")
    slab_rows = weight_term.shape[0] // (cycle_count * batch_count)
    reordered = weight_term.reshape(cycle_count, batch_count, slab_rows, -1).transpose(1, 0, 2, 3)
    reordered = reordered.reshape(weight_term.shape[0], -1)
    partial_batch = lax.psum_scatter(
        reordered.astype(jnp.bfloat16), "fsdp", scatter_dimension=0, tiled=True
    )
    weight_gradient = lax.psum_scatter(partial_batch, "cp", scatter_dimension=0, tiled=True).astype(
        jnp.float32
    )
    return (
        projected[None],
        query_gradient[None],
        key_gradient[None],
        value_gradient[None],
        weight_gradient,
    )


MESH = pl.DeviceIdType.MESH


def remote(src, dst, send_sem, recv_sem, device):
    return pltpu.make_async_remote_copy(
        src_ref=src,
        dst_ref=dst,
        send_sem=send_sem,
        recv_sem=recv_sem,
        device_id=device,
        device_id_type=MESH,
    )


def rows_of(begin, count):
    return pl.ds(pl.multiple_of(begin, count), count)


def greet(devices):
    barrier = pltpu.get_barrier_semaphore()
    for device in devices:
        pl.semaphore_signal(barrier, inc=1, device_id=device, device_id_type=MESH)
    pl.semaphore_wait(barrier, len(devices))


def layer_kernel(
    n, q, k, v, up, w, allowed, proj, dq, dk, dv, wg,
    qh, kh, vh, ups, wall, prob, att, attended, dqh, dkh, dvh, dk_sum, dv_sum, dw_sum, dw, dwr,
    kt, vt, local_sem, heads_s, heads_r, out_s, out_r, ring_s, ring_r,
    part_s, part_r, cross_s, cross_r, relay_s, relay_r, ws, wr,
):
    me = lax.axis_index("cp")
    col = lax.axis_index("fsdp")
    partner = {"fsdp": col + 1 - 2 * lax.rem(col, 2)}
    cross_col = lax.rem(col + 2, 4)
    cross = {"fsdp": cross_col}
    tokens = up.shape[0]
    half = tokens // 2
    slab = w.shape[0]
    depth = n // 2
    zed, why = me // 2, lax.rem(me, 2)
    place = zed + why * (n - 1 - 2 * zed)

    def at_place(offset):
        r = lax.rem(place + offset + 2 * n, n)
        return 2 * r + (r // depth) * (2 * n - 1 - 4 * r)

    def head_cols(d):
        return rows_of(d * HEAD, HEAD)

    peers = [{"cp": lax.rem(me + i, n)} for i in range(1, n)]
    columns = [{"fsdp": lax.rem(col + j, 4)} for j in range(1, 4)]
    greet(peers + columns)

    def chunk_ref(which, owner):
        if which == 2:
            return wall.at[rows_of(owner * (4 * slab) + col * slab, slab)]
        return ups.at[rows_of(owner * tokens + which * half, half)]

    def own_ref(which):
        if which == 2:
            return w
        return up.at[rows_of(which * half, half)]

    sends = []
    toward = ({"cp": at_place(1)}, {"cp": at_place(-1)})

    def chunks_at(step, way):
        if step < depth:
            return (2, 0, 1)
        return (2, 0) if way == 0 else (1,)

    def ring_start(step, way, which):
        owner = at_place((1 - step) if way == 0 else (step - 1))
        source = own_ref(which) if step == 1 else chunk_ref(which, owner)
        copy = remote(
            source, chunk_ref(which, owner),
            ring_s.at[way, step, which], ring_r.at[way, step, which], toward[way],
        )
        copy.start()
        sends.append(copy)

    def ring_wait(step, way, which):
        owner = at_place(-step if way == 0 else step)
        block = chunk_ref(which, owner)
        remote(
            block, block, ring_s.at[way, step, which], ring_r.at[way, step, which], toward[way]
        ).wait_recv()

    spread = []

    def spread_weight(owner, source):
        slot = len(spread)
        spread.append(owner)
        block = chunk_ref(2, owner)
        for device, ss, rs in ((cross, cross_s, cross_r), (partner, part_s, part_r)):
            copy = remote(source, block, ss.at[slot], rs.at[slot], device)
            copy.start()
            sends.append(copy)

    for way in range(2):
        for which in chunks_at(1, way):
            ring_start(1, way, which)
    triples = ((q, qh), (k, kh), (v, vh))
    for i in range(1, n):
        d = lax.rem(me + i, n)
        for t, (a, b) in enumerate(triples):
            copy = remote(
                a.at[:, head_cols(d)], b.at[rows_of(me * tokens, tokens)],
                heads_s.at[t, i], heads_r.at[t, i], {"cp": d},
            )
            copy.start()
            sends.append(copy)
    own = [
        pltpu.make_async_copy(
            a.at[:, head_cols(me)], b.at[rows_of(me * tokens, tokens)], local_sem.at[t]
        )
        for t, (a, b) in enumerate(triples)
    ]
    own.append(pltpu.make_async_copy(up, ups.at[rows_of(me * tokens, tokens)], local_sem.at[3]))
    own.append(pltpu.make_async_copy(w, chunk_ref(2, me), local_sem.at[4]))
    for copy in own:
        copy.start()
    spread_weight(me, w)
    bf16, f32 = jnp.bfloat16, jnp.float32
    nt = (((1,), (1,)), ((), ()))
    near = partner["fsdp"]
    far = lax.rem(near + 2, 4)

    def relay(slot):
        block = wall.at[rows_of(spread[slot] * (4 * slab) + cross_col * slab, slab)]
        remote(block, block, cross_s.at[slot], cross_r.at[slot], cross).wait_recv()
        copy = remote(block, block, relay_s.at[slot], relay_r.at[slot], partner)
        copy.start()
        sends.append(copy)

    def weight_wait(slot):
        for other, ss, rs in ((near, part_s, part_r), (far, relay_s, relay_r)):
            block = wall.at[rows_of(spread[slot] * (4 * slab) + other * slab, slab)]
            remote(block, block, ss.at[slot], rs.at[slot], partner).wait_recv()

    def advance(step):
        for way in range(2):
            for which in chunks_at(step, way):
                ring_wait(step, way, which)
                if step < depth and which in chunks_at(step + 1, way):
                    ring_start(step + 1, way, which)
                if which == 2:
                    owner = at_place(-step if way == 0 else step)
                    spread_weight(owner, chunk_ref(2, owner))

    def out_send(t, i, source, target):
        d = lax.rem(me + i, n)
        copy = remote(
            source.at[rows_of(d * tokens, tokens)], target.at[:, head_cols(me)],
            out_s.at[t, i], out_r.at[t, i], {"cp": d},
        )
        copy.start()
        sends.append(copy)

    def out_wait(t, target):
        for i in range(1, n):
            source = lax.rem(me + n - i, n)
            block = target.at[:, head_cols(source)]
            remote(block, block, out_s.at[t, i], out_r.at[t, i], {"cp": source}).wait_recv()

    advance(1)
    relay(0)
    for i in range(1, n):
        source = lax.rem(me + n - i, n)
        for t, (a, b) in enumerate(triples):
            block = b.at[rows_of(source * tokens, tokens)]
            remote(block, block, heads_s.at[t, i], heads_r.at[t, i], {"cp": source}).wait_recv()
    for copy in own:
        copy.wait()
    kt[...] = kh[...].astype(f32).T.astype(bf16)
    vt[...] = vh[...].astype(f32).T.astype(bf16)
    dk_sum[...] = jnp.zeros_like(dk_sum)
    dv_sum[...] = jnp.zeros_like(dv_sum)
    dw_sum[...] = jnp.zeros_like(dw_sum)

    def forward(o, carry):
        rows = rows_of(o * tokens, tokens)
        scores = lax.dot_general(kh[...], qh[rows], nt, preferred_element_type=f32) * (1.0 / HEAD)
        scores = jnp.where(allowed[:, rows].astype(f32) > 0.5, scores, lowest)
        terms = jnp.exp(scores - scores.max(0, keepdims=True))
        probability = terms * (1.0 / terms.sum(0, keepdims=True))
        prob[:, rows] = probability
        att_t = jnp.dot(vt[...], probability.astype(bf16), preferred_element_type=f32)
        att[rows] = att_t.T.astype(bf16)
        return carry

    lax.fori_loop(0, n, forward, 0)
    weight_wait(0)
    for i in range(1, n):
        out_send(0, i, att, attended)
    attended[:, head_cols(me)] = att[rows_of(me * tokens, tokens)]

    def backward(o):
        rows = rows_of(o * tokens, tokens)
        up_rows = ups[rows]
        ga = lax.dot_general(
            up_rows, wall[rows_of(me * HEAD, HEAD)], nt, preferred_element_type=f32
        ).astype(bf16)
        att_rows = att[rows]
        delta = (att_rows.astype(f32) * ga.astype(f32)).T.sum(0, keepdims=True)
        dprob = lax.dot_general(vh[...], ga, nt, preferred_element_type=f32)
        probability = prob[:, rows]
        ds = (probability * (dprob - delta) * (1.0 / HEAD)).astype(bf16)
        dqh[rows] = jnp.dot(kt[...], ds, preferred_element_type=f32).T.astype(bf16)
        dk_sum[...] += jnp.dot(ds, qh[rows], preferred_element_type=f32)
        dv_sum[...] += jnp.dot(probability.astype(bf16), ga, preferred_element_type=f32)
        dw_sum[...] += lax.dot_general(
            att_rows, up_rows, (((0,), (0,)), ((), ())), preferred_element_type=f32
        )

    backward(me)
    for step in range(2, depth + 1):
        advance(step)
        for slot in range(2 * step - 3, 2 * step - 1):
            relay(slot)
        backward(at_place(1 - step))
        backward(at_place(step - 1))
    backward(at_place(depth))
    dkh[...] = dk_sum[...].astype(bf16)
    dvh[...] = dv_sum[...].astype(bf16)
    dw[...] = dw_sum[...].astype(bf16)
    triples_out = ((dkh, dk), (dvh, dv), (dqh, dq))
    mine = rows_of(me * tokens, tokens)
    for t, (a, b) in enumerate(triples_out):
        b[:, head_cols(me)] = a[mine]
        for i in range(1, n):
            out_send(t + 1, i, a, b)
    for j in range(1, 4):
        g = lax.rem(col + j, 4)
        copy = remote(dw.at[rows_of(g * slab, slab)], dwr.at[j], ws.at[j], wr.at[j], {"fsdp": g})
        copy.start()
        sends.append(copy)
    relay(len(spread) - 1)
    for slot in range(1, len(spread)):
        weight_wait(slot)
    out_wait(0, attended)
    width = math.gcd(proj.shape[1], 512)

    def project(i, carry):
        cols = rows_of(i * width, width)
        proj[:, cols] = jnp.dot(
            attended[...], wall[:, cols], preferred_element_type=f32
        ).astype(bf16)
        return carry

    lax.fori_loop(0, proj.shape[1] // width, project, 0)
    for j in range(1, 4):
        block = dwr.at[j]
        remote(block, block, ws.at[j], wr.at[j], columns[j - 1]).wait_recv()
    total = dw[rows_of(col * slab, slab)].astype(f32)
    for j in range(1, 4):
        total = total + dwr[j].astype(f32)
    wg[...] = total
    for t, (a, b) in enumerate(triples_out):
        out_wait(t + 1, b)
    for copy in sends:
        copy.wait_send()


def by_heads(query_states, key_states, value_states, span_order, block_mask, output_weight, upstream):
    n = lax.axis_size("cp")
    m = lax.axis_size("fsdp")
    tokens, width = query_states.shape[1:]
    length = tokens * n
    model = upstream.shape[2]
    slab = output_weight.shape[0]
    span_rows = tokens // 2
    bf16, f32 = jnp.bfloat16, jnp.float32
    shape = jax.ShapeDtypeStruct
    vmem = pl.BlockSpec(memory_space=pltpu.VMEM)
    dma = pltpu.SemaphoreType.DMA
    half = n // 2
    positions = (
        span_order[:, None] * span_rows + jnp.arange(span_rows, dtype=jnp.int32)[None, :]
    ).reshape(-1)
    spans = span_order.shape[0]
    member = (
        jnp.arange(length, dtype=jnp.int32)[:, None] // span_rows
        == jnp.arange(spans, dtype=jnp.int32)[None, :]
    ).astype(bf16)
    span_ok = storage_mask(span_order, block_mask).astype(bf16)
    key_side = lax.dot_general(member, span_ok, (((1,), (1,)), ((), ())), preferred_element_type=bf16)
    seen = lax.dot_general(key_side, member, (((1,), (1,)), ((), ())), preferred_element_type=f32)
    allowed = ((seen > 0.5) & (positions[:, None] <= positions[None, :])).astype(bf16)
    head_array = pltpu.VMEM((length, HEAD), bf16)
    head_sum = pltpu.VMEM((length, HEAD), f32)
    projected, dq, dk, dv, weight_gradient = pl.pallas_call(
        lambda *refs: layer_kernel(n, *refs),
        out_shape=(shape((tokens, model), bf16),)
        + (shape((tokens, width), bf16),) * 3
        + (shape((slab, model), f32),),
        in_specs=[vmem] * 6,
        out_specs=(vmem,) * 5,
        scratch_shapes=[
            head_array, head_array, head_array,
            pltpu.VMEM((length, model), bf16), pltpu.VMEM((width, model), bf16),
            pltpu.VMEM((length, length), f32), head_array, pltpu.VMEM((tokens, width), bf16),
            head_array, head_array, head_array, head_sum, head_sum,
            pltpu.VMEM((HEAD, model), f32), pltpu.VMEM((HEAD, model), bf16),
            pltpu.VMEM((m, slab, model), bf16),
            pltpu.VMEM((HEAD, length), bf16), pltpu.VMEM((HEAD, length), bf16),
            dma((5,)), dma((3, n)), dma((3, n)), dma((4, n)), dma((4, n)),
            dma((2, half + 1, 3)), dma((2, half + 1, 3)),
        ]
        + [dma((n,))] * 6 + [dma((m,))] * 2,
        compiler_params=pltpu.CompilerParams(
            collective_id=0, has_side_effects=True, vmem_limit_bytes=48 << 20
        ),
        name="layer",
    )(query_states[0], key_states[0], value_states[0], upstream[0], output_weight, allowed)
    return (projected[None], dq[None], dk[None], dv[None], weight_gradient)


def solution(mesh):
    fits = mesh.shape["cp"] == HEADS and mesh.shape["fsdp"] == 4
    return jax.shard_map(
        by_heads if fits else local,
        mesh=mesh,
        in_specs=(
            P("fsdp", "cp", None),
            P("fsdp", "cp", None),
            P("fsdp", "cp", None),
            P(),
            P(),
            P(("cp", "fsdp"), None),
            P("fsdp", "cp", None),
        ),
        out_specs=(
            P("fsdp", "cp", None),
            P("fsdp", "cp", None),
            P("fsdp", "cp", None),
            P("fsdp", "cp", None),
            P(("cp", "fsdp"), None),
        ),
        check_vma=False,
    )
```

```python
import math

import jax
import jax.numpy as jnp
from jax import lax
from jax.experimental import pallas as pl
from jax.experimental.pallas import tpu as pltpu
from jax.sharding import PartitionSpec as P

HEADS = 8
HEAD = 128


lowest = -1e30


def split_heads(row_block):
    return row_block.reshape(row_block.shape[0], HEADS, HEAD)


def pair_scores(query_rows, key_rows):
    return jnp.einsum(
        "qhd,khd->hqk",
        split_heads(query_rows),
        split_heads(key_rows),
        preferred_element_type=jnp.float32,
    ) * (1.0 / HEAD)


def storage_mask(span_order, block_mask):
    span_count = span_order.shape[0]
    onehot = (span_order[:, None] == jnp.arange(span_count, dtype=jnp.int32)[None, :]).astype(
        jnp.float32
    )
    permuted = jnp.dot(jnp.dot(onehot, block_mask.astype(jnp.float32)), onehot.T)
    return permuted > 0.5


def allowed_block(span_ok, positions, query_begin, query_total, key_begin, key_total, span_rows):
    span_sub = lax.dynamic_slice(
        span_ok,
        (query_begin // span_rows, key_begin // span_rows),
        (query_total // span_rows, key_total // span_rows),
    )
    spread = jnp.broadcast_to(
        span_sub[:, None, :, None],
        (query_total // span_rows, span_rows, key_total // span_rows, span_rows),
    )
    spread = spread.reshape(query_total, key_total)
    query_pos = lax.dynamic_slice_in_dim(positions, query_begin, query_total)
    key_pos = lax.dynamic_slice_in_dim(positions, key_begin, key_total)
    return spread & (key_pos[None, :] <= query_pos[:, None])


def local_terms(query_rows, grad_rows, log_rows, delta_rows, key_rows, value_rows, allowed):
    scores = pair_scores(query_rows, key_rows)
    probability = jnp.where(allowed[None], jnp.exp(scores - log_rows[..., None]), 0.0)
    dprob = jnp.einsum(
        "qhd,khd->hqk",
        split_heads(grad_rows),
        split_heads(value_rows),
        preferred_element_type=jnp.float32,
    )
    dscores = (probability * (dprob - delta_rows[..., None]) * (1.0 / HEAD)).astype(jnp.bfloat16)
    return (probability, dscores)


def local(query_states, key_states, value_states, span_order, block_mask, output_weight, upstream):
    query_rows = query_states[0]
    key_local = key_states[0]
    value_local = value_states[0]
    upstream_rows = upstream[0]
    tokens = query_rows.shape[0]
    span_rows = tokens // 2
    positions = (
        span_order[:, None] * span_rows + jnp.arange(span_rows, dtype=jnp.int32)[None, :]
    ).reshape(-1)
    span_ok = storage_mask(span_order, block_mask)
    own_start = lax.axis_index("cp") * tokens
    key_all, value_all = (
        lax.all_gather(key_local, "cp", axis=0, tiled=True),
        lax.all_gather(value_local, "cp", axis=0, tiled=True),
    )
    weight = lax.all_gather(output_weight, ("cp", "fsdp"), axis=0, tiled=True)
    length = key_all.shape[0]
    key_block = math.gcd(length, 512)
    block_count = length // key_block
    block_steps = jnp.arange(block_count, dtype=jnp.int32)

    def stats_step(running, step_index):
        key_begin = step_index * key_block
        key_rows = lax.dynamic_slice_in_dim(key_all, key_begin, key_block)
        allowed = allowed_block(
            span_ok, positions, own_start, tokens, key_begin, key_block, span_rows
        )
        maxima, totals = running
        scores = pair_scores(query_rows, key_rows)
        masked = jnp.where(allowed[None], scores, lowest)
        new_max = jnp.maximum(maxima, masked.max(-1))
        exp_terms = jnp.where(allowed[None], jnp.exp(scores - new_max[..., None]), 0.0)
        return ((new_max, totals * jnp.exp(maxima - new_max) + exp_terms.sum(-1)), None)

    stat_start = (
        jnp.full((HEADS, tokens), lowest, jnp.float32),
        jnp.zeros((HEADS, tokens), jnp.float32),
    )
    (maxima, totals), _ = lax.scan(stats_step, stat_start, block_steps)
    log_total = maxima + jnp.log(totals)

    def output_step(attn_sum, step_index):
        key_begin = step_index * key_block
        key_rows = lax.dynamic_slice_in_dim(key_all, key_begin, key_block)
        value_rows = lax.dynamic_slice_in_dim(value_all, key_begin, key_block)
        allowed = allowed_block(
            span_ok, positions, own_start, tokens, key_begin, key_block, span_rows
        )
        scores = pair_scores(query_rows, key_rows)
        probability = jnp.where(allowed[None], jnp.exp(scores - log_total[..., None]), 0.0)
        return (
            attn_sum
            + jnp.einsum(
                "hqk,khd->qhd",
                probability.astype(jnp.bfloat16),
                split_heads(value_rows),
                preferred_element_type=jnp.float32,
            ),
            None,
        )

    zero_heads = jnp.zeros((tokens, HEADS, HEAD), jnp.float32)
    attn_sum, _ = lax.scan(output_step, zero_heads, block_steps)
    attended = lax.optimization_barrier(attn_sum.reshape(tokens, -1).astype(jnp.bfloat16))
    projected = jnp.dot(attended, weight, preferred_element_type=jnp.float32).astype(jnp.bfloat16)
    grad_attended = lax.dot_general(
        upstream_rows, weight, (((1,), (1,)), ((), ())), preferred_element_type=jnp.float32
    ).astype(jnp.bfloat16)
    grad_attended = lax.optimization_barrier(grad_attended)
    weight_term = lax.dot_general(
        attended, upstream_rows, (((0,), (0,)), ((), ())), preferred_element_type=jnp.float32
    )
    row_delta = (
        (grad_attended.astype(jnp.float32) * attended.astype(jnp.float32))
        .reshape(tokens, HEADS, HEAD)
        .sum(-1)
    )
    delta_heads = row_delta.T

    def query_step(grad_sum, step_index):
        key_begin = step_index * key_block
        key_rows = lax.dynamic_slice_in_dim(key_all, key_begin, key_block)
        value_rows = lax.dynamic_slice_in_dim(value_all, key_begin, key_block)
        allowed = allowed_block(
            span_ok, positions, own_start, tokens, key_begin, key_block, span_rows
        )
        probability, dscores = local_terms(
            query_rows, grad_attended, log_total, delta_heads, key_rows, value_rows, allowed
        )
        return (
            grad_sum
            + jnp.einsum(
                "hqk,khd->qhd", dscores, split_heads(key_rows), preferred_element_type=jnp.float32
            ),
            None,
        )

    query_sum, _ = lax.scan(query_step, zero_heads, block_steps)
    query_gradient = query_sum.reshape(tokens, -1).astype(jnp.bfloat16)
    log_all, delta_all = (
        lax.all_gather(log_total.T, "cp", axis=0, tiled=True),
        lax.all_gather(row_delta, "cp", axis=0, tiled=True),
    )
    sums_now = (zero_heads, zero_heads)
    query_piece = lax.all_gather(query_rows, "cp", axis=0, tiled=True)
    grad_piece = lax.all_gather(grad_attended, "cp", axis=0, tiled=True)
    row_count = query_piece.shape[0]
    sources = row_count // tokens
    group_size = math.gcd(sources, max(1, 512 // tokens))
    group_rows = group_size * tokens

    def group_step(running, step_index):
        offset = step_index * group_rows
        query_group = lax.dynamic_slice_in_dim(query_piece, offset, group_rows)
        grad_group = lax.dynamic_slice_in_dim(grad_piece, offset, group_rows)
        log_group = lax.dynamic_slice_in_dim(log_all, offset, group_rows).T
        delta_group = lax.dynamic_slice_in_dim(delta_all, offset, group_rows).T
        allowed = allowed_block(
            span_ok, positions, offset, group_rows, own_start, tokens, span_rows
        )
        key_sum, value_sum = running
        probability, dscores = local_terms(
            query_group, grad_group, log_group, delta_group, key_local, value_local, allowed
        )
        probability_low = probability.astype(jnp.bfloat16).reshape(
            HEADS, group_size, tokens, tokens
        )
        dscores_group = dscores.reshape(HEADS, group_size, tokens, tokens)
        qsplit = query_group.reshape(group_size, tokens, HEADS, HEAD)
        gsplit = grad_group.reshape(group_size, tokens, HEADS, HEAD)
        key_part = jnp.einsum(
            "hgqk,gqhd->gkhd", dscores_group, qsplit, preferred_element_type=jnp.float32
        ).astype(jnp.bfloat16)
        value_part = jnp.einsum(
            "hgqk,gqhd->gkhd", probability_low, gsplit, preferred_element_type=jnp.float32
        ).astype(jnp.bfloat16)
        key_part, value_part = lax.optimization_barrier((key_part, value_part))
        return (
            (
                key_sum + key_part.astype(jnp.float32).sum(0),
                value_sum + value_part.astype(jnp.float32).sum(0),
            ),
            None,
        )

    sums_now, _ = lax.scan(group_step, sums_now, jnp.arange(sources // group_size, dtype=jnp.int32))
    key_sum, value_sum = sums_now
    key_gradient = key_sum.reshape(tokens, -1).astype(jnp.bfloat16)
    value_gradient = value_sum.reshape(tokens, -1).astype(jnp.bfloat16)
    cycle_count = lax.axis_size("cp")
    batch_count = lax.axis_size("fsdp")
    slab_rows = weight_term.shape[0] // (cycle_count * batch_count)
    reordered = weight_term.reshape(cycle_count, batch_count, slab_rows, -1).transpose(1, 0, 2, 3)
    reordered = reordered.reshape(weight_term.shape[0], -1)
    partial_batch = lax.psum_scatter(
        reordered.astype(jnp.bfloat16), "fsdp", scatter_dimension=0, tiled=True
    )
    weight_gradient = lax.psum_scatter(partial_batch, "cp", scatter_dimension=0, tiled=True).astype(
        jnp.float32
    )
    return (
        projected[None],
        query_gradient[None],
        key_gradient[None],
        value_gradient[None],
        weight_gradient,
    )


MESH = pl.DeviceIdType.MESH


def remote(src, dst, send_sem, recv_sem, device):
    return pltpu.make_async_remote_copy(
        src_ref=src,
        dst_ref=dst,
        send_sem=send_sem,
        recv_sem=recv_sem,
        device_id=device,
        device_id_type=MESH,
    )


def rows_of(begin, count):
    return pl.ds(pl.multiple_of(begin, count), count)


def greet(devices):
    barrier = pltpu.get_barrier_semaphore()
    for device in devices:
        pl.semaphore_signal(barrier, inc=1, device_id=device, device_id_type=MESH)
    pl.semaphore_wait(barrier, len(devices))


def layer_kernel(
    n, q, k, v, up, w, allowed, proj, dq, dk, dv, wg,
    qh, kh, vh, ups, wall, prob, att, attended, dqh, dkh, dvh, dk_sum, dv_sum, dw_sum, dw, dwr,
    kt, vt, local_sem, heads_s, heads_r, out_s, out_r, ring_s, ring_r,
    part_s, part_r, cross_s, cross_r, relay_s, relay_r, ws, wr,
):
    me = lax.axis_index("cp")
    col = lax.axis_index("fsdp")
    partner = {"fsdp": col + 1 - 2 * lax.rem(col, 2)}
    cross_col = lax.rem(col + 2, 4)
    cross = {"fsdp": cross_col}
    tokens = up.shape[0]
    half = tokens // 2
    slab = w.shape[0]
    depth = n // 2
    zed, why = me // 2, lax.rem(me, 2)
    place = zed + why * (n - 1 - 2 * zed)

    def at_place(offset):
        r = lax.rem(place + offset + 2 * n, n)
        return 2 * r + (r // depth) * (2 * n - 1 - 4 * r)

    def head_cols(d):
        return rows_of(d * HEAD, HEAD)

    peers = [{"cp": lax.rem(me + i, n)} for i in range(1, n)]
    columns = [{"fsdp": lax.rem(col + j, 4)} for j in range(1, 4)]
    greet(peers + columns)

    def chunk_ref(which, owner):
        if which == 2:
            return wall.at[rows_of(owner * (4 * slab) + col * slab, slab)]
        return ups.at[rows_of(owner * tokens + which * half, half)]

    def own_ref(which):
        if which == 2:
            return w
        return up.at[rows_of(which * half, half)]

    sends = []
    toward = ({"cp": at_place(1)}, {"cp": at_place(-1)})

    def chunks_at(step, way):
        if step < depth:
            return (2, 0, 1)
        return (2, 0) if way == 0 else (1,)

    def ring_start(step, way, which):
        owner = at_place((1 - step) if way == 0 else (step - 1))
        source = own_ref(which) if step == 1 else chunk_ref(which, owner)
        copy = remote(
            source, chunk_ref(which, owner),
            ring_s.at[way, step, which], ring_r.at[way, step, which], toward[way],
        )
        copy.start()
        sends.append(copy)

    def ring_wait(step, way, which):
        owner = at_place(-step if way == 0 else step)
        block = chunk_ref(which, owner)
        remote(
            block, block, ring_s.at[way, step, which], ring_r.at[way, step, which], toward[way]
        ).wait_recv()

    spread = []

    def spread_weight(owner, source):
        slot = len(spread)
        spread.append(owner)
        block = chunk_ref(2, owner)
        for device, ss, rs in ((cross, cross_s, cross_r), (partner, part_s, part_r)):
            copy = remote(source, block, ss.at[slot], rs.at[slot], device)
            copy.start()
            sends.append(copy)

    for way in range(2):
        for which in chunks_at(1, way):
            ring_start(1, way, which)
    triples = ((q, qh), (k, kh), (v, vh))
    for i in range(1, n):
        d = lax.rem(me + i, n)
        for t, (a, b) in enumerate(triples):
            copy = remote(
                a.at[:, head_cols(d)], b.at[rows_of(me * tokens, tokens)],
                heads_s.at[t, i], heads_r.at[t, i], {"cp": d},
            )
            copy.start()
            sends.append(copy)
    own = [
        pltpu.make_async_copy(
            a.at[:, head_cols(me)], b.at[rows_of(me * tokens, tokens)], local_sem.at[t]
        )
        for t, (a, b) in enumerate(triples)
    ]
    own.append(pltpu.make_async_copy(up, ups.at[rows_of(me * tokens, tokens)], local_sem.at[3]))
    own.append(pltpu.make_async_copy(w, chunk_ref(2, me), local_sem.at[4]))
    for copy in own:
        copy.start()
    spread_weight(me, w)
    bf16, f32 = jnp.bfloat16, jnp.float32
    nt = (((1,), (1,)), ((), ()))
    near = partner["fsdp"]
    far = lax.rem(near + 2, 4)

    def relay(slot):
        block = wall.at[rows_of(spread[slot] * (4 * slab) + cross_col * slab, slab)]
        remote(block, block, cross_s.at[slot], cross_r.at[slot], cross).wait_recv()
        copy = remote(block, block, relay_s.at[slot], relay_r.at[slot], partner)
        copy.start()
        sends.append(copy)

    def weight_wait(slot):
        for other, ss, rs in ((near, part_s, part_r), (far, relay_s, relay_r)):
            block = wall.at[rows_of(spread[slot] * (4 * slab) + other * slab, slab)]
            remote(block, block, ss.at[slot], rs.at[slot], partner).wait_recv()

    def advance(step, chunks):
        for which in chunks:
            for way in range(2):
                if which not in chunks_at(step, way):
                    continue
                ring_wait(step, way, which)
                if step < depth and which in chunks_at(step + 1, way):
                    ring_start(step + 1, way, which)
                if which == 2:
                    owner = at_place(-step if way == 0 else step)
                    spread_weight(owner, chunk_ref(2, owner))

    def out_send(t, i, source, target):
        d = lax.rem(me + i, n)
        copy = remote(
            source.at[rows_of(d * tokens, tokens)], target.at[:, head_cols(me)],
            out_s.at[t, i], out_r.at[t, i], {"cp": d},
        )
        copy.start()
        sends.append(copy)

    def out_wait(t, target):
        for i in range(1, n):
            source = lax.rem(me + n - i, n)
            block = target.at[:, head_cols(source)]
            remote(block, block, out_s.at[t, i], out_r.at[t, i], {"cp": source}).wait_recv()

    advance(1, (2, 0, 1))
    relay(0)
    for i in range(1, n):
        source = lax.rem(me + n - i, n)
        for t, (a, b) in enumerate(triples):
            block = b.at[rows_of(source * tokens, tokens)]
            remote(block, block, heads_s.at[t, i], heads_r.at[t, i], {"cp": source}).wait_recv()
    for copy in own:
        copy.wait()
    kt[...] = kh[...].astype(f32).T.astype(bf16)
    vt[...] = vh[...].astype(f32).T.astype(bf16)
    dk_sum[...] = jnp.zeros_like(dk_sum)
    dv_sum[...] = jnp.zeros_like(dv_sum)
    dw_sum[...] = jnp.zeros_like(dw_sum)

    def forward(o, carry):
        rows = rows_of(o * tokens, tokens)
        scores = lax.dot_general(kh[...], qh[rows], nt, preferred_element_type=f32) * (1.0 / HEAD)
        scores = jnp.where(allowed[:, rows].astype(f32) > 0.5, scores, lowest)
        terms = jnp.exp(scores - scores.max(0, keepdims=True))
        probability = terms * (1.0 / terms.sum(0, keepdims=True))
        prob[:, rows] = probability
        att_t = jnp.dot(vt[...], probability.astype(bf16), preferred_element_type=f32)
        att[rows] = att_t.T.astype(bf16)
        return carry

    lax.fori_loop(0, n, forward, 0)
    weight_wait(0)
    for i in range(1, n):
        out_send(0, i, att, attended)
    attended[:, head_cols(me)] = att[rows_of(me * tokens, tokens)]

    def backward(o):
        rows = rows_of(o * tokens, tokens)
        up_rows = ups[rows]
        ga = lax.dot_general(
            up_rows, wall[rows_of(me * HEAD, HEAD)], nt, preferred_element_type=f32
        ).astype(bf16)
        att_rows = att[rows]
        delta = (att_rows.astype(f32) * ga.astype(f32)).T.sum(0, keepdims=True)
        dprob = lax.dot_general(vh[...], ga, nt, preferred_element_type=f32)
        probability = prob[:, rows]
        ds = (probability * (dprob - delta) * (1.0 / HEAD)).astype(bf16)
        dqh[rows] = jnp.dot(kt[...], ds, preferred_element_type=f32).T.astype(bf16)
        dk_sum[...] += jnp.dot(ds, qh[rows], preferred_element_type=f32)
        dv_sum[...] += jnp.dot(probability.astype(bf16), ga, preferred_element_type=f32)
        dw_sum[...] += lax.dot_general(
            att_rows, up_rows, (((0,), (0,)), ((), ())), preferred_element_type=f32
        )

    def query_send(o):
        i = lax.rem(o + n - me, n)
        copy = remote(
            dqh.at[rows_of(o * tokens, tokens)], dq.at[:, head_cols(me)],
            out_s.at[3, i], out_r.at[3, i], {"cp": o},
        )
        copy.start()
        sends.append(copy)

    backward(me)
    for step in range(2, depth + 1):
        advance(step, (2, 0))
        if step > 2:
            for offset in (2 - step, step - 2):
                query_send(at_place(offset))
        relay(2 * step - 3)
        backward(at_place(1 - step))
        advance(step, (1,))
        relay(2 * step - 2)
        backward(at_place(step - 1))
    backward(at_place(depth))
    dkh[...] = dk_sum[...].astype(bf16)
    dvh[...] = dv_sum[...].astype(bf16)
    dw[...] = dw_sum[...].astype(bf16)
    triples_out = ((dkh, dk), (dvh, dv), (dqh, dq))
    mine = rows_of(me * tokens, tokens)
    for t, (a, b) in enumerate(triples_out):
        b[:, head_cols(me)] = a[mine]
        if t < 2:
            for i in range(1, n):
                out_send(t + 1, i, a, b)
    for offset in (1 - depth, depth - 1, depth):
        query_send(at_place(offset))
    for j in range(1, 4):
        g = lax.rem(col + j, 4)
        copy = remote(dw.at[rows_of(g * slab, slab)], dwr.at[j], ws.at[j], wr.at[j], {"fsdp": g})
        copy.start()
        sends.append(copy)
    relay(len(spread) - 1)
    for slot in range(1, len(spread)):
        weight_wait(slot)
    out_wait(0, attended)
    width = math.gcd(proj.shape[1], 512)

    def project(i, carry):
        cols = rows_of(i * width, width)
        proj[:, cols] = jnp.dot(
            attended[...], wall[:, cols], preferred_element_type=f32
        ).astype(bf16)
        return carry

    lax.fori_loop(0, proj.shape[1] // width, project, 0)
    for j in range(1, 4):
        block = dwr.at[j]
        remote(block, block, ws.at[j], wr.at[j], columns[j - 1]).wait_recv()
    total = dw[rows_of(col * slab, slab)].astype(f32)
    for j in range(1, 4):
        total = total + dwr[j].astype(f32)
    wg[...] = total
    for t, (a, b) in enumerate(triples_out):
        out_wait(t + 1, b)
    for copy in sends:
        copy.wait_send()


def by_heads(query_states, key_states, value_states, span_order, block_mask, output_weight, upstream):
    n = lax.axis_size("cp")
    m = lax.axis_size("fsdp")
    tokens, width = query_states.shape[1:]
    length = tokens * n
    model = upstream.shape[2]
    slab = output_weight.shape[0]
    span_rows = tokens // 2
    bf16, f32 = jnp.bfloat16, jnp.float32
    shape = jax.ShapeDtypeStruct
    vmem = pl.BlockSpec(memory_space=pltpu.VMEM)
    dma = pltpu.SemaphoreType.DMA
    half = n // 2
    positions = (
        span_order[:, None] * span_rows + jnp.arange(span_rows, dtype=jnp.int32)[None, :]
    ).reshape(-1)
    spans = span_order.shape[0]
    member = (
        jnp.arange(length, dtype=jnp.int32)[:, None] // span_rows
        == jnp.arange(spans, dtype=jnp.int32)[None, :]
    ).astype(bf16)
    span_ok = storage_mask(span_order, block_mask).astype(bf16)
    key_side = lax.dot_general(member, span_ok, (((1,), (1,)), ((), ())), preferred_element_type=bf16)
    seen = lax.dot_general(key_side, member, (((1,), (1,)), ((), ())), preferred_element_type=f32)
    allowed = ((seen > 0.5) & (positions[:, None] <= positions[None, :])).astype(bf16)
    head_array = pltpu.VMEM((length, HEAD), bf16)
    head_sum = pltpu.VMEM((length, HEAD), f32)
    projected, dq, dk, dv, weight_gradient = pl.pallas_call(
        lambda *refs: layer_kernel(n, *refs),
        out_shape=(shape((tokens, model), bf16),)
        + (shape((tokens, width), bf16),) * 3
        + (shape((slab, model), f32),),
        in_specs=[vmem] * 6,
        out_specs=(vmem,) * 5,
        scratch_shapes=[
            head_array, head_array, head_array,
            pltpu.VMEM((length, model), bf16), pltpu.VMEM((width, model), bf16),
            pltpu.VMEM((length, length), f32), head_array, pltpu.VMEM((tokens, width), bf16),
            head_array, head_array, head_array, head_sum, head_sum,
            pltpu.VMEM((HEAD, model), f32), pltpu.VMEM((HEAD, model), bf16),
            pltpu.VMEM((m, slab, model), bf16),
            pltpu.VMEM((HEAD, length), bf16), pltpu.VMEM((HEAD, length), bf16),
            dma((5,)), dma((3, n)), dma((3, n)), dma((4, n)), dma((4, n)),
            dma((2, half + 1, 3)), dma((2, half + 1, 3)),
        ]
        + [dma((n,))] * 6 + [dma((m,))] * 2,
        compiler_params=pltpu.CompilerParams(
            collective_id=0, has_side_effects=True, vmem_limit_bytes=48 << 20
        ),
        name="layer",
    )(query_states[0], key_states[0], value_states[0], upstream[0], output_weight, allowed)
    return (projected[None], dq[None], dk[None], dv[None], weight_gradient)


def solution(mesh):
    fits = mesh.shape["cp"] == HEADS and mesh.shape["fsdp"] == 4
    return jax.shard_map(
        by_heads if fits else local,
        mesh=mesh,
        in_specs=(
            P("fsdp", "cp", None),
            P("fsdp", "cp", None),
            P("fsdp", "cp", None),
            P(),
            P(),
            P(("cp", "fsdp"), None),
            P("fsdp", "cp", None),
        ),
        out_specs=(
            P("fsdp", "cp", None),
            P("fsdp", "cp", None),
            P("fsdp", "cp", None),
            P("fsdp", "cp", None),
            P(("cp", "fsdp"), None),
        ),
        check_vma=False,
    )
```
